128 devices in a mesh: space: 8 (over y_hi, x), dp: 16 (over y_lo, z, core).
Axes of the slice: x: 4, y: 4 (y_hi: 2, y_lo: 2; y = y_hi * 2 + y_lo), z: 4, core: 2. Of those that a mesh axis runs over, the one named last changes fastest.
Arguments:
- mixed_two: bfloat16 [16, 32, 180, 768], P('dp', 'space'), may hold values from -6 to 6
- input_two: bfloat16 [16, 32, 180, 768], P('dp', 'space'), may hold values from -6 to 6
- cotangent: bfloat16 [16, 32, 180, 768], P('dp', 'space'), may hold values from -6 to 6
- w_in_two: bfloat16 [3072, 768], replicated, may hold values from -0.21875 to 0.21875
- w_out_two: bfloat16 [3072, 768], replicated, may hold values from -0.109375 to 0.109375
- kernel_two: bfloat16 [9, 768], replicated, may hold values from -2 to 2
- mixed_one: bfloat16 [16, 32, 180, 768], P('dp', 'space'), may hold values from -6 to 6
- w_in_one: bfloat16 [3072, 768], replicated, may hold values from -0.21875 to 0.21875
- w_out_one: bfloat16 [3072, 768], replicated, may hold values from -0.109375 to 0.109375
- kernel_one: bfloat16 [9, 768], replicated, may hold values from -2 to 2
Outputs:
- input_grad: bfloat16 [16, 32, 180, 768], P('dp', 'space')
- grad_w_in: float32 [3072, 768], P('dp')
- grad_w_out: float32 [3072, 768], P('dp')
- grad_kernel: float32 [9, 768], replicated
The draws below stay inside these ranges and needn't reach their ends.
All inputs are finite; a program needn't handle non-finite values.
Results may differ from the reference program's by a relative error of at most 0.02.
Values may be sent and summed in bfloat16 or wider, within the bound.
No kernel may reach another device: no remote copies, remote signals or barrier semaphores. Data moves between devices by JAX's collectives and lax.ppermute only.
A program may use at most 192 MiB of HBM per device.

```python
import math
import jax
import jax.numpy as jnp
from jax import lax

D = 768
FF = 3072
LON = 180
LAT = 32
BATCH = 16
TAPS = 9


def shard_levels(stream_key, extent, cuts, smallest, top_value):
    loudness = 1.0
    for dim, parts in cuts:
        steps = jax.random.uniform(jax.random.fold_in(jax.random.fold_in(stream_key, 6), dim), (parts,), jnp.float32, smallest / len(cuts), top_value / len(cuts))
        loudness = loudness * jnp.repeat(jnp.exp(steps), extent[dim] // parts).reshape((-1,) + (1,) * (len(extent) - 1 - dim))
    return loudness


def bell_draw(key, dims, width, limit, shards=(), held_as=jnp.bfloat16):
    drawn = jax.random.normal(key, dims, jnp.float32) * width
    if len(shards) > 0:
        drawn = shard_levels(key, dims, shards, -0.22, 0.18) * drawn
    return jnp.clip(drawn, min=-limit, max=limit).astype(held_as)


def setup_inputs(seed: int = 0) -> dict:
    seeds = jax.random.split(jax.random.key(seed), 11)
    mixed_two = bell_draw(seeds[0], (BATCH, LAT, LON, D), 1.0, 6.0, ((0, 16), (1, 8)))
    input_two = bell_draw(seeds[1], (BATCH, LAT, LON, D), 1.0, 6.0, ((0, 16), (1, 8)))
    cotangent = bell_draw(seeds[2], (BATCH, LAT, LON, D), 1.0, 6.0, ((0, 16), (1, 8)))
    w_in_two = bell_draw(seeds[3], (FF, D), D ** -0.5, 0.21875)
    w_out_two = bell_draw(seeds[4], (FF, D), FF ** -0.5, 0.109375)
    kernel_two = bell_draw(seeds[5], (TAPS, D), 0.35, 2.0)
    mixed_one = bell_draw(seeds[6], (BATCH, LAT, LON, D), 1.0, 6.0, ((0, 16), (1, 8)))
    w_in_one = bell_draw(seeds[7], (FF, D), D ** -0.5, 0.21875)
    w_out_one = bell_draw(seeds[8], (FF, D), FF ** -0.5, 0.109375)
    kernel_one = bell_draw(seeds[9], (TAPS, D), 0.35, 2.0)
    return {"mixed_two": mixed_two, "input_two": input_two, "cotangent": cotangent, "w_in_two": w_in_two, "w_out_two": w_out_two, "kernel_two": kernel_two, "mixed_one": mixed_one, "w_in_one": w_in_one, "w_out_one": w_out_one, "kernel_one": kernel_one}


GELU_C = math.sqrt(2.0 / math.pi)
CONTRACT_LAST = (((1,), (1,)), ((), ()))
CONTRACT_FIRST = (((0,), (0,)), ((), ()))

def gelu_parts(preact):
    tanh_arg = GELU_C * (preact + 0.044715 * preact * preact * preact)
    tanh_val = jnp.tanh(tanh_arg)
    activation = 0.5 * preact * (1.0 + tanh_val)
    gelu_slope = 0.5 * (1.0 + tanh_val) + 0.5 * preact * (1.0 - tanh_val * tanh_val) * GELU_C * (1.0 + 3.0 * 0.044715 * preact * preact)
    return (activation, gelu_slope)

def pad_rows(field):
    return jnp.pad(field, ((0, 0), (1, 1), (0, 0), (0, 0)))

def conv_back(padded, kernel, band_rows):
    kernel_f = kernel.astype(jnp.float32)
    result = jnp.zeros(padded[:, 1:1 + band_rows].shape, jnp.float32)
    for lat_off in range(3):
        for lon_off in range(3):
            window = padded[:, 2 - lat_off:2 - lat_off + band_rows].astype(jnp.float32)
            result = result + kernel_f[3 * lat_off + lon_off] * jnp.roll(window, lon_off - 1, axis=2)
    return result

def kernel_terms(padded_in, mix_grad, band_rows):
    grad_f = mix_grad.astype(jnp.float32)
    collected = []
    for lat_off in range(3):
        for lon_off in range(3):
            window = jnp.roll(padded_in[:, lat_off:lat_off + band_rows], 1 - lon_off, axis=2)
            collected.append(lax.optimization_barrier(jnp.sum(window.astype(jnp.float32) * grad_f, axis=(0, 1, 2))))
    return jnp.stack(collected)

def reference(mixed_two, input_two, cotangent, w_in_two, w_out_two, kernel_two, mixed_one, w_in_one, w_out_one, kernel_one):

    def sample_pass(items):
        mixed_late, input_late, cot_late, mixed_early = [item[None] for item in items]
        shape4 = mixed_late.shape
        band_rows = shape4[1]
        channels = shape4[3]
        mixed_flat = mixed_late.reshape(-1, channels)
        cot_flat = cot_late.reshape(-1, channels)
        preact = lax.dot_general(mixed_flat, w_in_two, CONTRACT_LAST, preferred_element_type=jnp.float32)
        activation, gelu_slope = gelu_parts(preact)
        activation = activation.astype(jnp.bfloat16)
        hidden_grad = lax.dot_general(cot_flat, w_out_two, CONTRACT_LAST, preferred_element_type=jnp.float32)
        pre_grad = (hidden_grad * gelu_slope).astype(jnp.bfloat16)
        mix_grad = jnp.dot(pre_grad, w_in_two, preferred_element_type=jnp.float32).astype(jnp.bfloat16).reshape(shape4)
        out_term = lax.dot_general(activation, cot_flat, CONTRACT_FIRST, preferred_element_type=jnp.float32)
        in_term = lax.dot_general(pre_grad, mixed_flat, CONTRACT_FIRST, preferred_element_type=jnp.float32)
        taps_term = kernel_terms(pad_rows(input_late), mix_grad, band_rows)
        grad_two = (cot_late.astype(jnp.float32) + conv_back(pad_rows(mix_grad), kernel_two, band_rows)).astype(jnp.bfloat16)
        preact_early = lax.dot_general(mixed_early.reshape(-1, channels), w_in_one, CONTRACT_LAST, preferred_element_type=jnp.float32)
        unused_act, slope_early = gelu_parts(preact_early)
        hidden_early = lax.dot_general(grad_two.reshape(-1, channels), w_out_one, CONTRACT_LAST, preferred_element_type=jnp.float32)
        pre_early = (hidden_early * slope_early).astype(jnp.bfloat16)
        mix_early = jnp.dot(pre_early, w_in_one, preferred_element_type=jnp.float32).astype(jnp.bfloat16).reshape(shape4)
        grad_one = (grad_two.astype(jnp.float32) + conv_back(pad_rows(mix_early), kernel_one, band_rows)).astype(jnp.bfloat16)
        return (grad_one[0], in_term, out_term, taps_term)
    grad_one, in_terms, out_terms, tap_terms = lax.map(sample_pass, (mixed_two, input_two, cotangent, mixed_one))
    grad_w_in = lax.optimization_barrier(jnp.sum(in_terms, axis=0)) / BATCH
    grad_w_out = lax.optimization_barrier(jnp.sum(out_terms, axis=0)) / BATCH
    grad_kernel = lax.optimization_barrier(jnp.sum(tap_terms, axis=0)) / BATCH
    return (grad_one, grad_w_in, grad_w_out, grad_kernel)
```

```python
import functools
import math

import jax
import jax.numpy as jnp
from jax import lax
from jax.experimental import pallas as pl
from jax.experimental.pallas import tpu as pltpu
from jax.sharding import Mesh
from jax.sharding import PartitionSpec as P

SPACE = ("yh", "x")
DP = ("yl", "z", "c")

GELU_C = math.sqrt(2.0 / math.pi)
NT = (((1,), (1,)), ((), ()))
TN = (((0,), (0,)), ((), ()))
NN = (((1,), (0,)), ((), ()))

LON = 180
LONP = 192
CHUNKS = 4
VMEM_BIG = 56 * 1024 * 1024

PAIR2 = [(0, 1), (1, 0)]
PAIR_A = [(0, 1), (1, 0), (2, 3), (3, 2)]
PAIR_B = [(1, 2), (2, 1), (3, 0), (0, 3)]


def dot(a, b, dims):
    return lax.dot_general(a, b, dims, preferred_element_type=jnp.float32)


def gelu_both(p):
    p2 = p * p
    t = jnp.tanh(p * (GELU_C + (GELU_C * 0.044715) * p2))
    half = 0.5 * p
    act = half + half * t
    slope = 0.5 + 0.5 * t + half * (1.0 - t * t) * (GELU_C + (3.0 * 0.044715 * GELU_C) * p2)
    return act, slope


def params(limit=VMEM_BIG, sem=("arbitrary",)):
    return pltpu.CompilerParams(dimension_semantics=sem, vmem_limit_bytes=limit)


def full(shape):
    return pl.BlockSpec(shape, lambda *_: (0,) * len(shape))


def cost(flops, nbytes, trans=0):
    return pl.CostEstimate(flops=int(flops), bytes_accessed=int(nbytes), transcendentals=int(trans))


def pad_body(x_ref, c_ref, xo_ref, co_ref):
    for src, dst in ((x_ref, xo_ref), (c_ref, co_ref)):
        for r in range(src.shape[1]):
            dst[r * LONP + 176 : (r + 1) * LONP, :] = jnp.zeros((16, dst.shape[1]), dst.dtype)
            dst[r * LONP : r * LONP + LON, :] = src[0, r]


def pad_pair(x, c):
    _, rows, lon, ch = x.shape
    out = jax.ShapeDtypeStruct((rows * LONP, ch), x.dtype)
    bw = 256
    return pl.pallas_call(
        pad_body,
        grid=(ch // bw,),
        in_specs=[pl.BlockSpec((1, rows, lon, bw), lambda i: (0, 0, 0, i))] * 2,
        out_specs=[pl.BlockSpec((rows * LONP, bw), lambda i: (0, i))] * 2,
        out_shape=[out, out],
        compiler_params=params(),
        cost_estimate=cost(1e9, 5e6),
        name="pad_pair",
    )(x, c)


def slope_body(x_ref, w_ref, o_ref, xp, pre):
    @pl.when(pl.program_id(0) == 0)
    def _():
        for r in range(x_ref.shape[1]):
            xp[r * LONP + 176 : (r + 1) * LONP, :] = jnp.zeros((16, xp.shape[1]), xp.dtype)
            xp[r * LONP : r * LONP + LON, :] = x_ref[0, r]

    pre[...] = dot(w_ref[...], xp[...], NT)

    def strip(i, carry):
        sl = pl.ds(pl.multiple_of(i * 16, 16), 16)
        o_ref[sl, :] = gelu_both(pre[sl, :])[1].astype(o_ref.dtype)
        return carry

    lax.fori_loop(0, pre.shape[0] // 16, strip, 0)


def slope_one(x, w):
    _, rows, lon, ch = x.shape
    ff = w.shape[0]
    fb = 512
    tok = rows * LONP
    return pl.pallas_call(
        slope_body,
        grid=(ff // fb,),
        in_specs=[full(x.shape), pl.BlockSpec((fb, ch), lambda i: (i, 0))],
        out_specs=pl.BlockSpec((fb, tok), lambda i: (i, 0)),
        out_shape=jax.ShapeDtypeStruct((ff, tok), jnp.bfloat16),
        scratch_shapes=[pltpu.VMEM((tok, ch), jnp.bfloat16), pltpu.VMEM((fb, tok), jnp.float32)],
        compiler_params=params(),
        cost_estimate=cost(2 * ff * ch * tok * 1.5, 1e7, ff * tok),
        name="slope_one",
    )(x, w)


def chunk_body(order, inv_batch, ids, xa, xb, ca, cb, wi_ref, wo_ref, keep, send, preg, pre, hid, act):
    tok = xa.shape[0]
    rows = wi_ref.shape[4]
    fb = 8 * rows
    wi = wi_ref[...].reshape(fb, -1)
    wo = wo_ref[...].reshape(fb, -1)
    pre[:, :tok] = dot(wi, xa[...], NT)
    pre[:, tok:] = dot(wi, xb[...], NT)
    hid[:, :tok] = dot(wo, ca[...], NT)
    hid[:, tok:] = dot(wo, cb[...], NT)

    def strip(i, carry):
        sl = pl.ds(pl.multiple_of(i * 16, 16), 16)
        a, s = gelu_both(pre[sl, :])
        act[sl, :] = a.astype(act.dtype)
        preg[sl, :] = (hid[sl, :] * s).astype(preg.dtype)
        return carry

    lax.fori_loop(0, fb // 16, strip, 0)
    ch = xa.shape[1]
    pre[:, :ch] = dot(act[:, :tok], ca[...], NN) + dot(act[:, tok:], cb[...], NN)
    pre[:, ch:] = dot(preg[:, :tok], xa[...], NN) + dot(preg[:, tok:], xb[...], NN)
    mine = ids[1]
    for slot in range(4):
        z = order[slot]
        half = slot // 2

        def put(dst):
            for yl in range(2):
                base = (yl * 4 + z) * rows
                for t in range(2):
                    block = pre[base : base + rows, t * ch : (t + 1) * ch] * inv_batch
                    dst[slot % 2, yl, t] = block.astype(dst.dtype)

        pl.when(mine == half)(functools.partial(put, keep))
        pl.when(mine != half)(functools.partial(put, send))


def chunk_two(k, order, inv_batch, ids, xa, xb, ca, cb, wi6, wo6):
    tok, ch = xa.shape
    rows = wi6.shape[4]
    fb = 8 * rows
    wspec = pl.BlockSpec((2, 4, 1, 1, rows, ch), lambda i, s: (0, 0, s[0], k, 0, 0))
    half = jax.ShapeDtypeStruct((2, 2, 2, rows, ch), jnp.bfloat16)
    hspec = full(half.shape)
    return pl.pallas_call(
        functools.partial(chunk_body, order, inv_batch),
        grid_spec=pltpu.PrefetchScalarGridSpec(
            num_scalar_prefetch=1,
            grid=(1,),
            in_specs=[full(xa.shape)] * 4 + [wspec, wspec],
            out_specs=[hspec, hspec, full((fb, 2 * tok))],
            scratch_shapes=[
                pltpu.VMEM((fb, 2 * tok), jnp.float32),
                pltpu.VMEM((fb, 2 * tok), jnp.float32),
                pltpu.VMEM((fb, 2 * tok), jnp.bfloat16),
            ],
        ),
        out_shape=[half, half, jax.ShapeDtypeStruct((fb, 2 * tok), jnp.bfloat16)],
        compiler_params=params(),
        cost_estimate=cost(4 * 2 * fb * ch * 2 * tok * 1.4, 8e6, fb * 2 * tok),
        name=f"chunk_two_{k}",
    )(ids, xa, xb, ca, cb, wi6, wo6)


def mix_body(ids, *refs):
    pregs, wi_ref, out = refs[:CHUNKS], refs[CHUNKS], refs[CHUNKS + 1]
    rows = wi_ref.shape[4]
    total = None
    for k in range(CHUNKS):
        w = wi_ref[:, :, 0, k].reshape(8 * rows, -1)
        part = dot(pregs[k][...], w, TN)
        total = part if total is None else total + part
    out[...] = total.astype(out.dtype)


def mix_part(half, dtype, ids, pregs, wi6):
    fb, tok2 = pregs[0].shape
    tok = tok2 // 2
    rows, ch = wi6.shape[4], wi6.shape[5]
    tb = 256
    nb = tok // tb
    return pl.pallas_call(
        mix_body,
        grid_spec=pltpu.PrefetchScalarGridSpec(
            num_scalar_prefetch=1,
            grid=(nb,),
            in_specs=[pl.BlockSpec((fb, tb), lambda i, s: (0, half * nb + i))] * CHUNKS
            + [pl.BlockSpec((2, 4, 1, CHUNKS, rows, ch), lambda i, s: (0, 0, s[0], 0, 0, 0))],
            out_specs=pl.BlockSpec((tb, ch), lambda i, s: (i, 0)),
        ),
        out_shape=jax.ShapeDtypeStruct((tok, ch), dtype),
        compiler_params=params(),
        cost_estimate=cost(2 * fb * CHUNKS * ch * tok, 6e6),
        name=f"mix_part_{half}",
    )(ids, *pregs, wi6)


def fill_extended(ext, row, cells):
    ext[row, 8 : 8 + LON, :] = cells
    ext[row, 7:8, :] = cells[LON - 1 : LON]
    ext[row, 8 + LON : 9 + LON, :] = cells[0:1]


def conv_rows(ext, kern, row):
    total = None
    for a in range(3):
        for b in range(3):
            window = ext[row + 2 - a, 9 - b : 9 - b + LON, :]
            term = kern[3 * a + b : 3 * a + b + 1, :] * window
            total = term if total is None else total + term
    return total


def conv_two_body(mix, top, bot, cot, inp, kern_ref, out, terms, ext):
    rows = inp.shape[1]
    fill_extended(ext, 0, top[:LON, :].astype(jnp.float32))
    fill_extended(ext, rows + 1, bot[:LON, :].astype(jnp.float32))
    for r in range(rows):
        fill_extended(ext, r + 1, mix[r * LONP : r * LONP + LON, :].astype(jnp.float32))
    kern = kern_ref[...].astype(jnp.float32)
    sums = [None] * 9
    for r in range(rows):
        total = cot[0, r].astype(jnp.float32)
        cells = inp[0, r].astype(jnp.float32)
        acc = None
        for a in range(3):
            for b in range(3):
                window = ext[r + 2 - a, 9 - b : 9 - b + LON, :]
                term = kern[3 * a + b : 3 * a + b + 1, :] * window
                acc = term if acc is None else acc + term
                part = jnp.sum(cells * window, axis=0, keepdims=True)
                sums[3 * a + b] = part if sums[3 * a + b] is None else sums[3 * a + b] + part
        out[r * LONP + 176 : (r + 1) * LONP, :] = jnp.zeros((16, out.shape[1]), out.dtype)
        out[r * LONP : r * LONP + LON, :] = (total + acc).astype(out.dtype)
    terms[...] = jnp.zeros_like(terms)
    for t in range(9):
        terms[t : t + 1, :] = sums[t]


def conv_two(mix, top, bot, cot, inp, kern):
    _, rows, lon, ch = inp.shape
    bw = 128
    flat = pl.BlockSpec((rows * LONP, bw), lambda i: (0, i))
    edge = pl.BlockSpec((LONP, bw), lambda i: (0, i))
    grid4 = pl.BlockSpec((1, rows, lon, bw), lambda i: (0, 0, 0, i))
    return pl.pallas_call(
        conv_two_body,
        grid=(ch // bw,),
        in_specs=[flat, edge, edge, grid4, grid4, pl.BlockSpec((9, bw), lambda i: (0, i))],
        out_specs=[flat, pl.BlockSpec((16, bw), lambda i: (0, i))],
        out_shape=[
            jax.ShapeDtypeStruct((rows * LONP, ch), jnp.bfloat16),
            jax.ShapeDtypeStruct((16, ch), jnp.float32),
        ],
        scratch_shapes=[pltpu.VMEM((rows + 2, 208, bw), jnp.float32)],
        compiler_params=params(),
        cost_estimate=cost(4e9, 5e6),
        name="conv_two",
    )(mix, top, bot, cot, inp, kern)


def conv_one_body(mix, top, bot, base, kern_ref, out, ext):
    rows = out.shape[1]
    fill_extended(ext, 0, top[:LON, :].astype(jnp.float32))
    fill_extended(ext, rows + 1, bot[:LON, :].astype(jnp.float32))
    for r in range(rows):
        fill_extended(ext, r + 1, mix[r * LONP : r * LONP + LON, :].astype(jnp.float32))
    kern = kern_ref[...].astype(jnp.float32)
    for r in range(rows):
        cells = base[r * LONP : r * LONP + LON, :].astype(jnp.float32)
        out[0, r] = (cells + conv_rows(ext, kern, r)).astype(out.dtype)


def conv_one(mix, top, bot, base, kern, shape):
    _, rows, lon, ch = shape
    bw = 128
    flat = pl.BlockSpec((rows * LONP, bw), lambda i: (0, i))
    edge = pl.BlockSpec((LONP, bw), lambda i: (0, i))
    return pl.pallas_call(
        conv_one_body,
        grid=(ch // bw,),
        in_specs=[flat, edge, edge, flat, pl.BlockSpec((9, bw), lambda i: (0, i))],
        out_specs=pl.BlockSpec((1, rows, lon, bw), lambda i: (0, 0, 0, i)),
        out_shape=jax.ShapeDtypeStruct(shape, jnp.bfloat16),
        scratch_shapes=[pltpu.VMEM((rows + 2, 208, bw), jnp.float32)],
        compiler_params=params(),
        cost_estimate=cost(3e9, 5e6),
        name="conv_one",
    )(mix, top, bot, base, kern)


def block_one_body(g, wo_ref, wi_ref, slope, out, acc):
    hid = dot(wo_ref[...], g[...], NT)
    pre = (hid * slope[...].astype(jnp.float32)).astype(jnp.bfloat16)
    part = dot(pre, wi_ref[...], TN)
    step = pl.program_id(0)

    @pl.when(step == 0)
    def _():
        acc[...] = part

    @pl.when(step > 0)
    def _():
        acc[...] += part

    @pl.when(step == pl.num_programs(0) - 1)
    def _():
        out[...] = acc[...].astype(out.dtype)


def block_one(g, wo, wi, slope):
    tok, ch = g.shape
    ff = wo.shape[0]
    fb = 512
    wspec = pl.BlockSpec((fb, ch), lambda i: (i, 0))
    return pl.pallas_call(
        block_one_body,
        grid=(ff // fb,),
        in_specs=[full(g.shape), wspec, wspec, pl.BlockSpec((fb, tok), lambda i: (i, 0))],
        out_specs=full((tok, ch)),
        out_shape=jax.ShapeDtypeStruct((tok, ch), jnp.bfloat16),
        scratch_shapes=[pltpu.VMEM((tok, ch), jnp.float32)],
        compiler_params=params(),
        cost_estimate=cost(4 * ff * ch * tok, 1.5e7),
        name="block_one",
    )(g, wo, wi, slope)


def halos(mix):
    count = lax.axis_size(SPACE)
    last = mix[mix.shape[0] - LONP :]
    first = mix[:LONP]
    top = lax.ppermute(last, SPACE, [(i, i + 1) for i in range(count - 1)])
    bot = lax.ppermute(first, SPACE, [(i + 1, i) for i in range(count - 1)])
    return top, bot


def add_round(a, b):
    return (a.astype(jnp.float32) + b.astype(jnp.float32)).astype(jnp.bfloat16)


def z_halving(keep, send, first, second, position):
    got = lax.ppermute(send, "z", first)

    def at(arr, i):
        return lax.dynamic_index_in_dim(arr, i, 0, keepdims=False)

    out = add_round(at(keep, 1 - position), at(got, 1 - position))
    back = lax.ppermute(out, "z", second)
    mine = at(keep, position).astype(jnp.float32) + at(got, position).astype(jnp.float32)
    return (mine + back.astype(jnp.float32)).astype(jnp.bfloat16)


def pair_sum(x, axis, pairs):
    return x + lax.ppermute(x, axis, pairs)


def shards(
    mixed_two,
    input_two,
    cotangent,
    w_in_two,
    w_out_two,
    kernel_two,
    mixed_one,
    w_in_one,
    w_out_one,
    kernel_one,
):
    shape4 = mixed_two.shape
    ff, ch = w_in_two.shape
    inv_batch = 1.0 / (shape4[0] * lax.axis_size(DP))
    owners = lax.axis_size(DP)
    rows = ff // owners // CHUNKS
    c = lax.axis_index("c")
    z = lax.axis_index("z")

    xa, ca = pad_pair(mixed_two, cotangent)
    xb = lax.ppermute(xa, "c", PAIR2)
    cb = lax.ppermute(ca, "c", PAIR2)
    slope = slope_one(mixed_one, w_in_one)

    wi6 = w_in_two.reshape(2, 4, 2, CHUNKS, rows, ch)
    wo6 = w_out_two.reshape(2, 4, 2, CHUNKS, rows, ch)
    class_a = ((z + 1) // 2) % 2
    class_b = z // 2
    place_a = jnp.where(class_a == 0, jnp.where(z == 3, 1, 0), jnp.where(z == 2, 1, 0))
    place_b = z % 2
    ids_a = jnp.stack([c, class_a]).astype(jnp.int32)
    ids_b = jnp.stack([c, class_b]).astype(jnp.int32)

    pregs, sums = [], []
    for k in range(CHUNKS):
        flavor_a = k % 2 == 0
        order = (0, 3, 1, 2) if flavor_a else (0, 1, 2, 3)
        ids = ids_a if flavor_a else ids_b
        keep, send, preg = chunk_two(k, order, inv_batch, ids, xa, xb, ca, cb, wi6, wo6)
        pregs.append(preg)
        first, second = (PAIR_A, PAIR_B) if flavor_a else (PAIR_B, PAIR_A)
        sums.append(z_halving(keep, send, first, second, place_a if flavor_a else place_b))

    other = lax.ppermute(mix_part(1, jnp.bfloat16, ids_a, pregs, wi6), "c", PAIR2)
    own = mix_part(0, jnp.float32, ids_a, pregs, wi6)
    mix_grad = (own + other.astype(jnp.float32)).astype(jnp.bfloat16)
    top, bot = halos(mix_grad)
    grad_two, terms = conv_two(mix_grad, top, bot, cotangent, input_two, kernel_two)
    mix_early = block_one(grad_two, w_out_one, w_in_one, slope)
    top1, bot1 = halos(mix_early)
    grad_one = conv_one(mix_early, top1, bot1, grad_two, kernel_one, shape4)

    terms = pair_sum(terms * inv_batch, "c", PAIR2)
    terms = pair_sum(terms, "z", PAIR_A)
    terms = pair_sum(terms, "z", PAIR_B)

    group = ("yl", "yh", "x")
    members = lax.axis_size(group)
    copies = lax.axis_size(SPACE)
    piece = 2 * 2 * rows // copies
    results = []
    for part in range(2):
        pair = jnp.stack([sums[2 * part], sums[2 * part + 1]], axis=1)
        pieces = pair.reshape(members, piece, ch)
        if part == 1:
            extra = jnp.broadcast_to(terms.astype(jnp.bfloat16)[None], (members, 16, ch))
            pieces = jnp.concatenate([pieces, extra], axis=1)
        arrived = lax.all_to_all(pieces, group, 0, 0, tiled=True)
        results.append(arrived.astype(jnp.float32).sum(axis=0))
    grad_kernel = results[1][piece : piece + 9]
    mine = jnp.concatenate([results[0], results[1][:piece]], axis=0).astype(jnp.bfloat16)
    spread = jnp.broadcast_to(mine[None], (copies,) + mine.shape)
    every = lax.all_to_all(spread, SPACE, 0, 0, tiled=True)
    every = every.reshape(2, 2, 2, 2, piece, ch).astype(jnp.float32)
    every = every.transpose(1, 3, 0, 2, 4, 5).reshape(2, ff // owners, ch)
    return (grad_one, every[1], every[0], grad_kernel)


def solution(mesh):
    finer = Mesh(mesh.devices.reshape(2, 4, 2, 4, 2), ("yh", "x", "yl", "z", "c"))
    banded = P(DP, SPACE, None, None)
    return jax.shard_map(
        shards,
        mesh=finer,
        in_specs=(banded, banded, banded, P(), P(), P(), banded, P(), P(), P()),
        out_specs=(banded, P(DP, None), P(DP, None), P()),
        check_vma=False,
    )
```
